32 devices in a mesh: grp: 2 (over y), vec: 4 (over z), occ: 2 (over x), wlk: 2 (over core).
Axes of the slice: x: 2, y: 2, z: 4, core: 2. Of those that a mesh axis runs over, the one named last changes fastest.
Arguments:
- chol_half: bfloat16 [256, 256, 2048], P(('grp', 'vec'), 'occ'), parts along dimension 0, may hold values from -0.046875 to 0.046875
- theta: bfloat16 [8, 2048, 256], P(('grp', 'wlk'), 'vec', 'occ'), parts along dimension 0, may hold values from -6 to 6
Outputs:
- theta_grad: float32 [8, 2048, 256], P(('grp', 'wlk'), 'vec', 'occ'), parts along dimension 0
The draws below stay inside these ranges and needn't reach their ends.
There are 2 independent parts, one for each index of `grp`. The reference program is written for one: setup_inputs(seed, part) draws one part's arguments, and reference() takes and returns one part's arrays. A program takes and returns all parts, laid end to end along the dimension named above; each array names one. Nothing has to cross between parts.
All inputs are finite; a program needn't handle non-finite values.
Results may differ from the reference program's by a relative error of at most 0.0042.
Values may be sent and summed in bfloat16 or wider, within the bound.
A program may use at most 64 MiB of HBM per device.

```python
import jax
import jax.numpy as jnp
from jax import lax

M = 2048
O = 256
NCHOL = 128
W = 4


def steps_of(own_key, shape, cuts, least, largest):
    loudness, own = 1.0, jax.random.fold_in(own_key, 6)
    for axis_at, shards_of in cuts:
        steps = jnp.exp(jax.random.uniform(jax.random.fold_in(own, axis_at), (shards_of,), jnp.float32, least / len(cuts), largest / len(cuts)))
        loudness = loudness * jnp.repeat(steps, shape[axis_at] // shards_of).reshape([-1 if axis == axis_at else 1 for axis in range(len(shape))])
    return loudness


def scatter_about(rng, shape, scale, reach, shards=(), kind=jnp.bfloat16):
    loudness = steps_of(rng, shape, shards, -0.22, 0.18) if shards else 1.0
    drawn = jax.random.normal(rng, shape, jnp.float32) * scale * loudness
    return jnp.minimum(jnp.maximum(drawn, -reach), reach).astype(kind)


def setup_inputs(seed: int = 0, part: int = 0) -> dict:
    key_list = jax.random.split(jax.random.key(seed), 3)
    own_keys = jax.random.split(jax.random.fold_in(key_list[2], part), 3)
    return {
        "chol_half": scatter_about(own_keys[0], (NCHOL, O, M), (7 * M) ** -0.5, 0.046875, ((0, 4), (1, 2))),
        "theta": scatter_about(own_keys[1], (W, M, O), 1.0, 6.0, ((0, 2), (1, 4), (2, 2))),
    }


def reference(chol_half, theta):
    walkers = theta.shape[0]

    def add_vector(carry, factor):
        grads = []
        for walker in range(walkers):
            amplitudes = jnp.dot(factor, theta[walker], preferred_element_type=jnp.float32).astype(jnp.bfloat16)
            grads.append(jnp.dot(factor.T, amplitudes.T, preferred_element_type=jnp.float32))
        return carry + jnp.stack(grads), None

    initial = jnp.zeros((walkers, M, O), jnp.float32)
    total, unused = lax.scan(add_vector, initial, chol_half)
    return -total
```

```python
import functools

import jax
import jax.numpy as jnp
from jax import lax
from jax.experimental import pallas as pl
from jax.experimental.pallas import tpu as pltpu
from jax.sharding import PartitionSpec as P

MESH = pl.DeviceIdType.MESH
F32 = jnp.float32
BF16 = jnp.bfloat16


def kernel(dims, chol, theta, out, cv, tho, thp, asend, arecv, adiag, acc, gs, gf, gc, gr, gown, xs, xr,
           csem, txs, txr, ags, agr, ass, asr, gss, gsr, xss, xsr):
    G, R, M, W, Q, CH, NQ, pieces, parts = dims
    z = lax.axis_index("vec")
    partner = {"occ": 1 - lax.axis_index("occ")}
    side = z // 2
    near, edge = 1 + side, 3 * side
    far, end = 3 - near, 3 - edge
    inner = z == near
    outer = z == edge
    mate = near + edge - z
    mine = pl.ds(pl.multiple_of(z * Q, Q), Q)
    GC = G // CH
    QC = Q // NQ

    drains = []

    def remote(src, dst, ss, rs, to):
        return pltpu.make_async_remote_copy(src_ref=src, dst_ref=dst, send_sem=ss, recv_sem=rs, device_id=to, device_id_type=MESH)

    def on(s):
        return {"vec": s}

    def c_copy(c):
        part = pl.ds(c * GC, GC)
        return pltpu.make_async_copy(chol.at[part], cv.at[part], csem.at[c])

    for c in range(CH):
        c_copy(c).start()

    barrier = pltpu.get_barrier_semaphore()
    pl.semaphore_signal(barrier, inc=1, device_id=partner, device_id_type=MESH)
    for k in range(1, 4):
        pl.semaphore_signal(barrier, inc=1, device_id=on(lax.rem(z + k, 4)), device_id_type=MESH)
    acc[...] = jnp.zeros_like(acc)
    for w in range(W):
        tho[w, mine] = theta[w]
    pl.semaphore_wait(barrier, 4)

    def rows_of(s, q, n):
        size = Q // n
        return pl.ds(pl.multiple_of(s * Q + q * size, size), size)

    def theta_x(w, q, n, source=None):
        source = z if source is None else source
        rows = rows_of(source, q, n)
        src = theta.at[w, pl.ds(q * (Q // n), Q // n)] if source is z else tho.at[w, rows]
        return remote(src, thp.at[w, rows], txs.at[w, q, source], txr.at[w, q, source], partner)

    def cross(w, q, n, source=None):
        theta_x(w, q, n, source).start()
        drains.append(theta_x(w, q, n, source).wait_send)

    class Gather:
        def __init__(self, s, buf, w, n):
            self.s, self.buf, self.w, self.n = s, buf, w, n

        def copy(self, q, kind, source, to):
            ref = self.buf.at[self.w, rows_of(source, q, self.n)]
            src = theta.at[self.w, pl.ds(q * (Q // self.n), Q // self.n)] if source is z and self.buf is tho else ref
            return remote(src, ref, ags.at[self.s, q, kind], agr.at[self.s, q, source], on(to))

        def start(self, q=0):
            self.copy(q, 0, z, mate).start()
            self.copy(q, 1, z, far).start()
            pl.when(inner)(lambda: self.copy(q, 2, z, end).start())
            drains.append(lambda: self.drain(q))

        def relay(self, q=0):
            @pl.when(inner)
            def _():
                self.copy(q, 0, end, edge).wait_recv()
                self.copy(q, 3, end, edge).start()

        def wait(self, q=0):
            self.copy(q, 0, far, mate).wait_recv()
            self.copy(q, 0, mate, mate).wait_recv()
            pl.when(outer)(lambda: self.copy(q, 0, end, mate).wait_recv())

        def drain(self, q):
            self.copy(q, 0, z, mate).wait_send()
            self.copy(q, 1, z, mate).wait_send()

            @pl.when(inner)
            def _():
                self.copy(q, 2, z, mate).wait_send()
                self.copy(q, 3, z, mate).wait_send()

    par0, own0, par1, own1 = Gather(0, thp, 0, NQ), Gather(1, tho, 0, NQ), Gather(2, thp, 1, 1), Gather(3, tho, 1, 1)

    NB = NQ // 2
    direct = range(NB, NQ)
    shared = range(NB)
    for q in (*direct, *shared):
        cross(0, q, NQ)
    for q in shared:
        own0.start(q)
    for q in direct:
        theta_x(0, q, NQ).wait_recv()
        par0.start(q)
    for q in shared:
        for source in (mate, far):
            own0.copy(q, 0, source, mate).wait_recv()
            cross(0, q, NQ, source)
        own0.relay(q)
        pl.when(inner)(lambda: theta_x(0, q, NQ, end).start())
    for q in direct:
        par0.relay(q)
    for q in shared:

        @pl.when(outer)
        def _():
            own0.copy(q, 0, end, mate).wait_recv()
            theta_x(0, q, NQ, end).start()

        drains.append(theta_x(0, q, NQ, end).wait_send)

    cross(1, 0, 1)
    for q in direct:
        own0.start(q)
    for q in direct:
        par0.wait(q)
    for q in shared:
        for source in (z, mate, far, end):
            theta_x(0, q, NQ, source).wait_recv()

    def a_copy(p, c):
        w, first, rows, n = pieces[p]
        part = (w, pl.ds(c * (G // n), G // n), pl.ds(first, rows))
        return remote(asend.at[part], arecv.at[part], ass.at[p, c], asr.at[p, c], partner)

    def send_amplitudes(p, lo=0, hi=None):
        w, first, rows, n = pieces[p]
        size = G // n

        @pl.loop(lo, n if hi is None else hi)
        def _(c):
            if p == 0:
                c_copy(c).wait()
            part = pl.ds(c * size, size)
            block = jnp.dot(cv[part, pl.ds(first, rows)].reshape(size * rows, M), thp[w], preferred_element_type=F32)
            asend[w, part, pl.ds(first, rows)] = block.astype(BF16).reshape(size, rows, R)
            a_copy(p, c).start()

        def drain():
            @pl.loop(lo, n if hi is None else hi)
            def _(c):
                a_copy(p, c).wait_send()

        drains.append(drain)

    GD = 2 * GC

    def diagonal(w):
        @pl.loop(0, G // GD)
        def _(c):
            part = pl.ds(c * GD, GD)
            block = jnp.dot(cv[part].reshape(GD * R, M), tho[w], preferred_element_type=F32)
            adiag[w, part] = block.astype(BF16).reshape(GD, R, R)

    def accumulate(stream, first, rows, block, part, size):
        lhs = jnp.concatenate([block[g] for g in range(size)], axis=1)
        for n in range(4):
            cols = pl.ds(n * Q, Q)
            acc[stream, pl.ds(first, rows), cols] += jnp.dot(
                lhs, cv[part, :, cols].reshape(size * R, Q), preferred_element_type=F32
            )

    def own_gradient(w):
        @pl.loop(0, G // GD)
        def _(c):
            part = pl.ds(c * GD, GD)
            accumulate(w, 0, R, adiag[w, part], part, GD)

    def swapped_gradient(p, lo=0, hi=None, step=1):
        w, first, rows, n = pieces[p]
        size = step * (G // n)

        @pl.loop(lo // step, (n if hi is None else hi) // step)
        def _(c):
            for k in range(step):
                a_copy(p, c * step + k).wait_recv()
            part = pl.ds(c * size, size)
            accumulate(W + w, first, rows, arecv[w, part, pl.ds(first, rows)], part, size)

    class Scatter:
        def __init__(self, e):
            self.e = e
            self.stream, self.first, self.rows = parts[e]
            self.span = pl.ds(self.first, self.rows)

        def own(self, d):
            return acc[self.stream, self.span, pl.ds(pl.multiple_of(d * Q, Q), Q)]

        def to_mate(self):
            at = (self.stream, 0, self.span)
            return remote(gs.at[at], gr.at[at], gss.at[self.e, 0], gsr.at[self.e, 0], on(mate))

        def to_near(self, k):
            return remote(gs.at[self.stream, 1 + k, self.span], gf.at[self.stream, k, self.span], gss.at[self.e, 1 + k], gsr.at[self.e, 1 + k], on(near))

        def across(self, k, to):
            return remote(gc.at[self.stream, k, self.span], gr.at[self.stream, 1, self.span], gss.at[self.e, 3 + k], gsr.at[self.e, 3], on(to))

        def start(self):
            @pl.when(outer)
            def _():
                for k, d in enumerate((far, end)):
                    gs[self.stream, 1 + k, self.span] = self.own(d).astype(BF16)
                    self.to_near(k).start()

            gs[self.stream, 0, self.span] = self.own(mate).astype(BF16)
            self.to_mate().start()
            drains.append(self.drain)

        def relay(self):
            @pl.when(inner)
            def _():
                for k, d in enumerate((far, end)):
                    self.to_near(k).wait_recv()
                    gc[self.stream, k, self.span] = (self.own(d) + gf[self.stream, k, self.span].astype(F32)).astype(BF16)
                    self.across(k, d).start()

        def total(self):
            self.to_mate().wait_recv()
            self.across(0, far).wait_recv()
            return self.own(z) + gr[self.stream, 0, self.span].astype(F32) + gr[self.stream, 1, self.span].astype(F32)

        def drain(self):
            self.to_mate().wait_send()

            @pl.when(outer)
            def _():
                for k in range(2):
                    self.to_near(k).wait_send()

            @pl.when(inner)
            def _():
                for k in range(2):
                    self.across(k, far).wait_send()

    def x_copy(e):
        stream, first, rows = parts[e]
        at = (stream - W, pl.ds(first, rows))
        return remote(xs.at[at], xr.at[at], xss.at[e], xsr.at[e], partner)

    def finish(e):
        stream, first, rows = parts[e]
        total = scatters[e].total()
        if stream < W:
            gown[stream] = total
        else:
            xs[stream - W, pl.ds(first, rows)] = total.astype(BF16)
            x_copy(e).start()
            drains.append(x_copy(e).wait_send)

    scatters = [Scatter(e) for e in range(len(parts))]
    D0, D1, F0, Fa, Fb, Fc = range(6)

    send_amplitudes(0, 0, 3)
    for q in direct:
        own0.relay(q)
    theta_x(1, 0, 1).wait_recv()
    par1.start()
    send_amplitudes(0, 3, 8)
    for q in direct:
        own0.wait(q)
    diagonal(0)
    par1.relay()
    own1.start()
    own_gradient(0)
    scatters[D0].start()
    swapped_gradient(0, 0, 2, 2)
    par1.wait()
    send_amplitudes(1)
    swapped_gradient(0, 2, 4, 2)
    own1.relay()
    scatters[D0].relay()
    send_amplitudes(2)
    send_amplitudes(3)
    swapped_gradient(0, 4, 8, 2)
    scatters[F0].start()
    own1.wait()
    diagonal(1)
    own_gradient(1)
    scatters[D1].start()
    scatters[F0].relay()
    finish(D0)
    swapped_gradient(1)
    scatters[Fa].start()
    finish(F0)
    scatters[D1].relay()
    swapped_gradient(2)
    scatters[Fb].start()
    scatters[Fa].relay()
    finish(D1)
    swapped_gradient(3)
    scatters[Fc].start()
    scatters[Fb].relay()
    finish(Fa)
    finish(Fb)
    scatters[Fc].relay()
    finish(Fc)
    for e in (F0, Fa, Fb, Fc):
        x_copy(e).wait_recv()

    for w in range(W):
        out[w] = -(gown[w] + xr[w].astype(F32)).T

    for drain in drains:
        drain()


def fused(chol_half, theta):
    G, R, M = chol_half.shape
    W, Q, _ = theta.shape
    CH = 8
    NQ = 4
    H = R // 2
    pieces = ((0, 0, R, CH), (1, 0, H, 4), (1, H, H // 2, 2), (1, H + H // 2, H // 2, 4))
    parts = ((0, 0, R), (1, 0, R), (W, 0, R)) + tuple((W + 1, first, rows) for _, first, rows, _ in pieces[1:])
    dims = (G, R, M, W, Q, CH, NQ, pieces, parts)
    E, PC = len(parts), len(pieces)
    dma = pltpu.SemaphoreType.DMA
    return pl.pallas_call(
        functools.partial(kernel, dims),
        out_shape=jax.ShapeDtypeStruct((W, Q, R), F32),
        in_specs=[pl.BlockSpec(memory_space=pl.ANY), pl.BlockSpec(memory_space=pltpu.VMEM)],
        out_specs=pl.BlockSpec(memory_space=pltpu.VMEM),
        scratch_shapes=[
            pltpu.VMEM((G, R, M), BF16),
            pltpu.VMEM((W, M, R), BF16),
            pltpu.VMEM((W, M, R), BF16),
            pltpu.VMEM((W, G, R, R), BF16),
            pltpu.VMEM((W, G, R, R), BF16),
            pltpu.VMEM((W, G, R, R), BF16),
            pltpu.VMEM((2 * W, R, M), F32),
            pltpu.VMEM((2 * W, 3, R, Q), BF16),
            pltpu.VMEM((2 * W, 2, R, Q), BF16),
            pltpu.VMEM((2 * W, 2, R, Q), BF16),
            pltpu.VMEM((2 * W, 2, R, Q), BF16),
            pltpu.VMEM((W, R, Q), F32),
            pltpu.VMEM((W, R, Q), BF16),
            pltpu.VMEM((W, R, Q), BF16),
            dma((CH,)),
            dma((W, NQ, 4)),
            dma((W, NQ, 4)),
            dma((2 * W, NQ, 4)),
            dma((2 * W, NQ, 4)),
            dma((PC, CH)),
            dma((PC, CH)),
            dma((E, 5)),
            dma((E, 4)),
            dma((E,)),
            dma((E,)),
        ],
        compiler_params=pltpu.CompilerParams(collective_id=0, has_side_effects=True, vmem_limit_bytes=60 << 20),
    )(chol_half, theta)


def on_device(mesh, chol_half, theta):
    G, R, M = chol_half.shape
    nz = mesh.shape["vec"]
    fits = theta.shape[0] == 2 and G % 16 == 0 and R == 128 and theta.shape[1] % 512 == 0 and G * R * M <= 8 << 20
    if mesh.shape["occ"] == 2 and nz == 4 and fits:
        return fused(chol_half, theta)
    widened = lax.all_gather(theta, "occ", axis=2, tiled=True)
    amplitude_sums = jnp.einsum(
        "gip,wpj->wgij", chol_half, lax.all_gather(widened, "vec", axis=1, tiled=True), preferred_element_type=F32
    )
    amplitudes = amplitude_sums.astype(BF16)
    swapped = lax.all_to_all(amplitudes, "occ", split_axis=3, concat_axis=2, tiled=True)
    summed_rows = lax.psum_scatter(
        jnp.einsum("gap,wgba->pwb", chol_half, swapped, preferred_element_type=F32),
        "vec",
        scatter_dimension=0,
        tiled=True,
    )
    owned = lax.psum_scatter(summed_rows, "occ", scatter_dimension=2, tiled=True)
    return -jnp.transpose(owned, (1, 0, 2))


def solution(mesh):
    return jax.shard_map(
        functools.partial(on_device, mesh),
        mesh=mesh,
        in_specs=(P(("grp", "vec"), "occ", None), P(("grp", "wlk"), "vec", "occ")),
        out_specs=P(("grp", "wlk"), "vec", "occ"),
        check_vma=False,
    )
```

```python
import functools

import jax
import jax.numpy as jnp
from jax import lax
from jax.experimental import pallas as pl
from jax.experimental.pallas import tpu as pltpu
from jax.sharding import PartitionSpec as P

MESH = pl.DeviceIdType.MESH
F32 = jnp.float32
BF16 = jnp.bfloat16


def kernel(dims, chol, theta, out, cv, ov, th, asend, arecv, adiag, acc, gs, gf, gc, gr, gown, xs, xr,
           csem, tsem, osem, txs, txr, txq, ags, agq, agr, ass, asr, gss, gsr, xss, xsr):
    G, R, M, W, Q, CH, NQ, NB, pieces, parts = dims
    z = lax.axis_index("vec")
    partner = {"occ": 1 - lax.axis_index("occ")}
    side = z // 2
    near, edge = 1 + side, 3 * side
    far, end = 3 - near, 3 - edge
    core = lax.axis_index("wlk")
    inner = z == near
    outer = z == edge
    mate = near + edge - z
    mine = pl.ds(pl.multiple_of(z * Q, Q), Q)
    GC = G // CH
    QC = Q // NQ

    drains = []

    def remote(src, dst, ss, rs, to):
        return pltpu.make_async_remote_copy(src_ref=src, dst_ref=dst, send_sem=ss, recv_sem=rs, device_id=to, device_id_type=MESH)

    def on(s):
        return {"vec": s}

    def c_copy(c):
        part = pl.ds(c * GC, GC)
        return pltpu.make_async_copy(chol.at[part], cv.at[part], csem)

    OWN, OTHER = pl.ds(0, R), pl.ds(R, R)

    def t_copy(w):
        return pltpu.make_async_copy(theta.at[w], th.at[w, mine, OWN], tsem.at[w])

    for w in range(W):
        t_copy(w).start()

    barrier = pltpu.get_barrier_semaphore()
    greeted = [partner]
    for k in range(1, 4):
        greeted.append(on(lax.rem(z + k, 4)))
    for device in greeted:
        pl.semaphore_signal(barrier, inc=1, device_id=device, device_id_type=MESH)
    acc[...] = jnp.zeros_like(acc)
    pl.semaphore_wait(barrier, len(greeted))

    def rows_of(s, q, n):
        size = Q // n
        return pl.ds(pl.multiple_of(s * Q + q * size, size), size)

    def cross(w, rows):
        remote(th.at[w, rows, OWN], th.at[w, rows, OTHER], txs.at[w], txr.at[w], partner).start()

    def crossed(w, rows):
        rows = pl.ds(0, rows)
        return remote(th.at[w, rows, OWN], th.at[w, rows, OTHER], txs.at[w], txr.at[w], partner)

    def cross_first(q):
        rows = rows_of(z, q, NQ)
        return remote(th.at[0, rows, OWN], th.at[0, rows, OTHER], txs.at[0], txq.at[q], partner)

    class Gather:
        def __init__(self, s, columns, w, n):
            self.s, self.columns, self.w, self.n = s, columns, w, n

        def block(self, rows, recv, to):
            ref = th.at[self.w, rows, self.columns]
            return remote(ref, ref, ags.at[self.s], recv, on(to))

        def recv(self, q, kind):
            return agr.at[self.s, kind // 2] if self.n == 1 else agq.at[self.s - 2, q, kind]

        def copy(self, q, source, to, kind):
            return self.block(rows_of(source, q, self.n), self.recv(q, kind), to)

        def start(self, q=0):
            self.begin(q)
            drains.append(self.drain)

        def begin(self, q=0):
            own = functools.partial(self.copy, q, z)
            own(mate, 0).start()

            @pl.when(inner)
            def _():
                own(far, 1).start()
                own(end, 1).start()

            pl.when(outer)(lambda: own(far, 2).start())

        def arrive(self, q, source, kind):
            self.copy(q, source, mate, kind).wait_recv()

        def relay(self, q=0):
            @pl.when(inner)
            def _():
                self.arrive(q, end, 2)
                self.copy(q, end, edge, 2).start()

        def wait(self, q=0):
            if self.n == 1:
                self.block(pl.ds(0, 2 * Q), self.recv(0, 0), mate).wait_recv()
            else:
                self.arrive(q, mate, 0)
                self.arrive(q, far, 1)
            pl.when(outer)(lambda: self.arrive(q, end, 2))

        def drain(self):
            size = Q // self.n
            pl.when(inner)(lambda: self.block(pl.ds(0, 4 * size), self.recv(0, 0), mate).wait_send())
            pl.when(outer)(lambda: self.block(pl.ds(0, 2 * size), self.recv(0, 0), mate).wait_send())

    own0, par0, own1, par1 = Gather(2, OWN, 0, NQ), Gather(3, OTHER, 0, NQ), Gather(0, OWN, 1, 1), Gather(1, OTHER, 1, 1)
    direct, shared = range(NB, NQ), range(NB)

    t_copy(0).wait()
    for c in range(CH):
        c_copy(c).start()
    for q in direct:
        cross_first(q).start()
    for q in shared:
        own0.start(q)
        cross(0, rows_of(z, q, NQ))
    t_copy(1).wait()
    cross(1, mine)
    drains.append(crossed(0, Q + 3 * NB * (Q // NQ)).wait_send)
    drains.append(crossed(1, Q).wait_send)
    for q in direct:
        cross_first(q).wait_recv()
        par0.start(q)
    for q in shared:
        for kind, source in enumerate((mate, far)):
            own0.arrive(q, source, kind)
            cross(0, rows_of(source, q, NQ))
        own0.relay(q)
        pl.when(inner)(lambda: cross(0, rows_of(end, q, NQ)))
    for q in direct:
        par0.relay(q)
    for q in shared:

        @pl.when(outer)
        def _():
            own0.arrive(q, end, 2)
            cross(0, rows_of(end, q, NQ))

    for q in direct:
        own0.start(q)
    for q in direct:
        par0.wait(q)
    crossed(1, Q).wait_recv()
    par1.start()
    own1.start()
    pltpu.make_async_copy(chol, cv, csem).wait()
    crossed(0, 4 * NB * (Q // NQ)).wait_recv()

    def a_copy(p, c, count=1):
        w, first, rows, n, step = pieces[p]
        part = (w, pl.ds(c * (G // n), count * (G // n)), pl.ds(first, rows))
        return remote(asend.at[part], arecv.at[part], ass.at[p], asr.at[p, c // step], partner)

    def send_amplitudes(p, lo=0, hi=None, both=False):
        w, first, rows, n, step = pieces[p]
        size = G // n
        span = pl.ds(first, rows)

        @pl.loop(lo, n if hi is None else hi)
        def _(c):
            part = pl.ds(c * size, size)
            lhs = cv[part, span].reshape(size * rows, M)
            if both:
                block = jnp.dot(lhs, th[w], preferred_element_type=F32).astype(BF16)
                asend[w, part, span] = block[:, R:].reshape(size, rows, R)
                a_copy(p, c).start()
                adiag[w, part, span] = block[:, :R].reshape(size, rows, R)
            else:
                block = jnp.dot(lhs, th[w, :, OTHER], preferred_element_type=F32).astype(BF16)
                asend[w, part, span] = block.reshape(size, rows, R)
                a_copy(p, c).start()

        if lo == 0:
            drains.append(a_copy(p, 0, n).wait_send)

    GD = 2 * GC

    def diagonal(w, lo, hi):
        @pl.loop(lo, hi)
        def _(c):
            part = pl.ds(c * GD, GD)
            block = jnp.dot(cv[part].reshape(GD * R, M), th[w, :, OWN], preferred_element_type=F32)
            adiag[w, part] = block.astype(BF16).reshape(GD, R, R)

    def accumulate(stream, first, rows, block, part, size):
        lhs = jnp.concatenate([block[g] for g in range(size)], axis=1)
        for n in range(4):
            cols = pl.ds(n * Q, Q)
            acc[stream, pl.ds(first, rows), cols] += jnp.dot(
                lhs, cv[part, :, cols].reshape(size * R, Q), preferred_element_type=F32
            )

    def own_gradient(w):
        @pl.loop(0, G // GD)
        def _(c):
            part = pl.ds(c * GD, GD)
            accumulate(w, 0, R, adiag[w, part], part, GD)

    def swapped_gradient(p, lo=0, hi=None):
        w, first, rows, n, step = pieces[p]
        size = step * (G // n)

        @pl.loop(lo, n // step if hi is None else hi)
        def _(c):
            a_copy(p, c * step, step).wait_recv()
            part = pl.ds(c * size, size)
            accumulate(W + w, first, rows, arecv[w, part, pl.ds(first, rows)], part, size)

    class Scatter:
        def __init__(self, e):
            self.e = e
            self.stream, self.first, self.rows, self.direct = parts[e]
            self.span = pl.ds(self.first, self.rows)

        def own(self, d):
            return acc[self.stream, self.span, pl.ds(pl.multiple_of(d * Q, Q), Q)]

        def link(self, src, dst, k, to):
            return remote(src, dst, gss.at[self.e], gsr.at[self.e, k], on(to))

        def straight(self, k, to, slot=None):
            return self.link(gs.at[self.stream, k, self.span], gr.at[self.stream, k if slot is None else slot, self.span], 0, to)

        def to_near(self, k):
            return self.link(gs.at[self.stream, 1 + k, self.span], gf.at[self.stream, k, self.span], 1 + k, near)

        def across(self, k, to):
            return self.link(gc.at[self.stream, k, self.span], gr.at[self.stream, 1, self.span], 0, to)

        def arrived(self, count):
            return self.link(gs.at[self.stream, pl.ds(0, count), self.span], gr.at[self.stream, pl.ds(0, count), self.span], 0, mate)

        def to_owner(self, d):
            at = (self.stream, d, self.span)
            return remote(gs.at[at], gr.at[self.stream, z, self.span], gss.at[self.e], gsr.at[self.e, 0], {**partner, **on(d)})

        def to_owners(self):
            at = (self.stream, pl.ds(0, 4), self.span)
            return remote(gs.at[at], gr.at[at], gss.at[self.e], gsr.at[self.e, 0], partner)

        def start(self):
            if self.direct == 2:
                for d in range(4):
                    gs[self.stream, d, self.span] = self.own(d).astype(BF16)
                for k in (end, far, near, edge):
                    self.to_owner(k).start()
                drains.append(self.to_owners().wait_send)
                return
            if self.direct:
                for k, d in ((2, 3 - z), (1, 3 - mate), (0, mate)):
                    gs[self.stream, k, self.span] = self.own(d).astype(BF16)
                    self.straight(k, d).start()
            else:

                @pl.when(outer)
                def _():
                    for k, d in enumerate((far, end)):
                        gs[self.stream, 1 + k, self.span] = self.own(d).astype(BF16)
                        self.to_near(k).start()

                gs[self.stream, 0, self.span] = self.own(mate).astype(BF16)
                self.straight(0, mate).start()
            drains.append(self.arrived(3).wait_send)

        def relay(self):
            @pl.when(inner)
            def _():
                for k, d in enumerate((far, end)):
                    self.to_near(k).wait_recv()
                    gc[self.stream, k, self.span] = (self.own(d) + gf[self.stream, k, self.span].astype(F32)).astype(BF16)
                    self.across(k, d).start()

        def total(self):
            count = 3 if self.direct else 2
            self.arrived(count).wait_recv()
            total = self.own(z)
            for k in range(count):
                total += gr[self.stream, k, self.span].astype(F32)
            return total

    def x_copy(w, rows=None):
        if rows is None:
            rows = pl.ds(0, sum(size for stream, _, size, mode in parts if stream == W + w and mode < 2))
        return remote(xs.at[w, rows], xr.at[w, rows], xss.at[w], xsr.at[w], partner)

    def finish(e):
        stream, first, rows, _ = parts[e]
        total = scatters[e].total()
        if stream < W:
            gown[stream] = total
        else:
            w, span = stream - W, pl.ds(first, rows)
            xs[w, span] = total.astype(BF16)
            x_copy(w, span).start()
            if first == 0:
                drains.append(x_copy(w).wait_send)

    def settle(count=None):
        count = len(drains) if count is None else count
        for drain in drains[:count]:
            drain()
        del drains[:count]

    def store(w):
        x_copy(w).wait_recv()
        for e, (stream, first, rows, mode) in enumerate(parts):
            if stream == W + w:
                span = pl.ds(first, rows)
                if mode == 2:
                    scatters[e].to_owners().wait_recv()
                    for d in range(4):
                        gown[w, span] += gr[stream, d, span].astype(F32)
                else:
                    gown[w, span] += xr[w, span].astype(F32)
        ov[w] = -gown[w].T
        pltpu.make_async_copy(ov.at[w], out.at[w], osem).start()
        if w == 0:
            drains.append(pltpu.make_async_copy(ov, out, osem).wait)

    scatters = [Scatter(e) for e in range(len(parts))]
    D0, D1, F0, Fa, Fb, Fc = range(6)

    send_amplitudes(0, 0, 4, both=True)
    par1.relay()
    send_amplitudes(0, 4, 8, both=True)
    own1.relay()
    own_gradient(0)
    scatters[D0].start()
    swapped_gradient(0, 0, 1)
    par1.wait()
    own1.wait()
    send_amplitudes(1, both=True)
    scatters[D0].relay()
    swapped_gradient(0, 1, 2)
    send_amplitudes(2, both=True)
    send_amplitudes(3, both=True)
    own_gradient(1)
    scatters[D1].start()
    swapped_gradient(0, 2, 4)
    scatters[F0].start()
    old = len(drains)
    finish(D0)
    swapped_gradient(1, 0, 1)
    scatters[D1].relay()
    swapped_gradient(1, 1, 4)
    scatters[Fa].start()
    scatters[F0].relay()
    swapped_gradient(2)
    scatters[Fb].start()
    scatters[Fa].relay()
    swapped_gradient(3)
    scatters[Fc].start()
    settle(old)
    finish(D1)
    finish(F0)
    finish(Fa)
    finish(Fb)
    finish(Fc)
    store(0)
    store(1)
    settle()


def fused(chol_half, theta):
    G, R, M = chol_half.shape
    W, Q, _ = theta.shape
    CH = 8
    NQ, NB = 4, 4
    H = R // 4
    modes = (0, 1, 1)
    pieces = ((0, 0, R, CH, 2), (1, 0, 2 * H, 4, 1), (1, 2 * H, H, 4, 1), (1, 3 * H, H, 4, 1))
    parts = ((0, 0, R, 0), (1, 0, R, 0), (W, 0, R, 0)) + tuple(
        (W + 1, first, rows, mode) for (_, first, rows, _, _), mode in zip(pieces[1:], modes)
    )
    dims = (G, R, M, W, Q, CH, NQ, NB, pieces, parts)
    E, PC = len(parts), len(pieces)
    dma = pltpu.SemaphoreType.DMA
    return pl.pallas_call(
        functools.partial(kernel, dims),
        out_shape=jax.ShapeDtypeStruct((W, Q, R), F32),
        in_specs=[pl.BlockSpec(memory_space=pl.ANY)] * 2,
        out_specs=pl.BlockSpec(memory_space=pl.ANY),
        scratch_shapes=[
            pltpu.VMEM((G, R, M), BF16),
            pltpu.VMEM((W, Q, R), F32),
            pltpu.VMEM((W, M, 2 * R), BF16),
            pltpu.VMEM((W, G, R, R), BF16),
            pltpu.VMEM((W, G, R, R), BF16),
            pltpu.VMEM((W, G, R, R), BF16),
            pltpu.VMEM((2 * W, R, M), F32),
            pltpu.VMEM((2 * W, 4, R, Q), BF16),
            pltpu.VMEM((2 * W, 2, R, Q), BF16),
            pltpu.VMEM((2 * W, 2, R, Q), BF16),
            pltpu.VMEM((2 * W, 4, R, Q), BF16),
            pltpu.VMEM((W, R, Q), F32),
            pltpu.VMEM((W, R, Q), BF16),
            pltpu.VMEM((W, R, Q), BF16),
            dma,
            dma((W,)),
            dma,
            dma((W,)),
            dma((W,)),
            dma((NQ,)),
            dma((4,)),
            dma((2, NQ, 3)),
            dma((2, 2)),
            dma((PC,)),
            dma((PC, 4)),
            dma((E,)),
            dma((E, 3)),
            dma((W,)),
            dma((W,)),
        ],
        compiler_params=pltpu.CompilerParams(collective_id=0, has_side_effects=True, vmem_limit_bytes=60 << 20),
    )(chol_half, theta)


def on_device(mesh, chol_half, theta):
    G, R, M = chol_half.shape
    nz = mesh.shape["vec"]
    fits = theta.shape[0] == 2 and G % 16 == 0 and R == 128 and theta.shape[1] % 512 == 0 and G * R * M <= 8 << 20
    if mesh.shape["occ"] == 2 and nz == 4 and fits:
        return fused(chol_half, theta)
    widened = lax.all_gather(theta, "occ", axis=2, tiled=True)
    amplitude_sums = jnp.einsum(
        "gip,wpj->wgij", chol_half, lax.all_gather(widened, "vec", axis=1, tiled=True), preferred_element_type=F32
    )
    amplitudes = amplitude_sums.astype(BF16)
    swapped = lax.all_to_all(amplitudes, "occ", split_axis=3, concat_axis=2, tiled=True)
    summed_rows = lax.psum_scatter(
        jnp.einsum("gap,wgba->pwb", chol_half, swapped, preferred_element_type=F32),
        "vec",
        scatter_dimension=0,
        tiled=True,
    )
    owned = lax.psum_scatter(summed_rows, "occ", scatter_dimension=2, tiled=True)
    return -jnp.transpose(owned, (1, 0, 2))


def solution(mesh):
    return jax.shard_map(
        functools.partial(on_device, mesh),
        mesh=mesh,
        in_specs=(P(("grp", "vec"), "occ", None), P(("grp", "wlk"), "vec", "occ")),
        out_specs=P(("grp", "wlk"), "vec", "occ"),
        check_vma=False,
    )
```

```python
import functools

import jax
import jax.numpy as jnp
from jax import lax
from jax.experimental import pallas as pl
from jax.experimental.pallas import tpu as pltpu
from jax.sharding import PartitionSpec as P

MESH = pl.DeviceIdType.MESH
F32 = jnp.float32
BF16 = jnp.bfloat16


def kernel(dims, chol, theta, out, cv, th, asend, arecv, adiag, acc, gs, gf, gc, gr, gown, xs, xr,
           csem, tsem, txs, txr, txq, ags, agq, agr, ass, asr, gss, gsr, xss, xsr):
    G, R, M, W, Q, CH, NQ, NB, pieces, parts = dims
    z = lax.axis_index("vec")
    partner = {"occ": 1 - lax.axis_index("occ")}
    side = z // 2
    near, edge = 1 + side, 3 * side
    far, end = 3 - near, 3 - edge
    core = lax.axis_index("wlk")
    inner = z == near
    outer = z == edge
    mate = near + edge - z
    mine = pl.ds(pl.multiple_of(z * Q, Q), Q)
    GC = G // CH
    QC = Q // NQ

    drains = []

    def remote(src, dst, ss, rs, to):
        return pltpu.make_async_remote_copy(src_ref=src, dst_ref=dst, send_sem=ss, recv_sem=rs, device_id=to, device_id_type=MESH)

    def on(s):
        return {"vec": s}

    def c_copy(c):
        part = pl.ds(c * GC, GC)
        return pltpu.make_async_copy(chol.at[part], cv.at[part], csem)

    OWN, OTHER = pl.ds(0, R), pl.ds(R, R)

    def t_copy(w):
        return pltpu.make_async_copy(theta.at[w], th.at[w, mine, OWN], tsem.at[w])

    for w in range(W):
        t_copy(w).start()

    barrier = pltpu.get_barrier_semaphore()
    greeted = [partner]
    for k in range(1, 4):
        greeted.append(on(lax.rem(z + k, 4)))
    for device in greeted:
        pl.semaphore_signal(barrier, inc=1, device_id=device, device_id_type=MESH)
    pl.semaphore_wait(barrier, len(greeted))

    def rows_of(s, q, n):
        size = Q // n
        return pl.ds(pl.multiple_of(s * Q + q * size, size), size)

    def cross(w, rows):
        remote(th.at[w, rows, OWN], th.at[w, rows, OTHER], txs.at[w], txr.at[w], partner).start()

    def crossed(w, rows):
        rows = pl.ds(0, rows)
        return remote(th.at[w, rows, OWN], th.at[w, rows, OTHER], txs.at[w], txr.at[w], partner)

    def cross_first(q):
        rows = rows_of(z, q, NQ)
        return remote(th.at[0, rows, OWN], th.at[0, rows, OTHER], txs.at[0], txq.at[q], partner)

    class Gather:
        def __init__(self, s, columns, w, n):
            self.s, self.columns, self.w, self.n = s, columns, w, n

        def block(self, rows, recv, to):
            ref = th.at[self.w, rows, self.columns]
            return remote(ref, ref, ags.at[self.s], recv, on(to))

        def recv(self, q, kind):
            return agr.at[self.s, kind // 2] if self.n == 1 else agq.at[self.s - 2, q, kind]

        def copy(self, q, source, to, kind):
            return self.block(rows_of(source, q, self.n), self.recv(q, kind), to)

        def start(self, q=0):
            self.begin(q)
            drains.append(self.drain)

        def begin(self, q=0):
            own = functools.partial(self.copy, q, z)
            own(mate, 0).start()

            @pl.when(inner)
            def _():
                own(far, 1).start()
                own(end, 1).start()

            pl.when(outer)(lambda: own(far, 2).start())

        def arrive(self, q, source, kind):
            self.copy(q, source, mate, kind).wait_recv()

        def relay(self, q=0):
            @pl.when(inner)
            def _():
                self.arrive(q, end, 2)
                self.copy(q, end, edge, 2).start()

        def wait(self, q=0):
            if self.n == 1:
                self.block(pl.ds(0, 2 * Q), self.recv(0, 0), mate).wait_recv()
            else:
                self.arrive(q, mate, 0)
                self.arrive(q, far, 1)
            pl.when(outer)(lambda: self.arrive(q, end, 2))

        def drain(self):
            size = Q // self.n
            pl.when(inner)(lambda: self.block(pl.ds(0, 4 * size), self.recv(0, 0), mate).wait_send())
            pl.when(outer)(lambda: self.block(pl.ds(0, 2 * size), self.recv(0, 0), mate).wait_send())

    own0, par0, own1, par1 = Gather(2, OWN, 0, NQ), Gather(3, OTHER, 0, NQ), Gather(0, OWN, 1, 1), Gather(1, OTHER, 1, 1)
    direct, shared = range(NB, NQ), range(NB)

    t_copy(0).wait()
    for c in range(CH):
        c_copy(c).start()
    for q in direct:
        cross_first(q).start()
    for q in shared:
        own0.start(q)
        cross(0, rows_of(z, q, NQ))
    acc[...] = jnp.zeros_like(acc)
    t_copy(1).wait()
    cross(1, mine)
    drains.append(crossed(0, Q + 3 * NB * (Q // NQ)).wait_send)
    drains.append(crossed(1, Q).wait_send)
    for q in direct:
        cross_first(q).wait_recv()
        par0.start(q)
    for q in shared:
        for kind, source in enumerate((mate, far)):
            own0.arrive(q, source, kind)
            cross(0, rows_of(source, q, NQ))
        own0.relay(q)
        pl.when(inner)(lambda: cross(0, rows_of(end, q, NQ)))
    for q in direct:
        par0.relay(q)
    for q in shared:

        @pl.when(outer)
        def _():
            own0.arrive(q, end, 2)
            cross(0, rows_of(end, q, NQ))

    for q in direct:
        own0.start(q)
    for q in direct:
        par0.wait(q)
    pltpu.make_async_copy(chol, cv, csem).wait()
    crossed(0, 4 * NB * (Q // NQ)).wait_recv()

    def a_copy(p, c, count=1):
        w, first, rows, n, step = pieces[p]
        part = (w, pl.ds(c * (G // n), count * (G // n)), pl.ds(first, rows))
        return remote(asend.at[part], arecv.at[part], ass.at[p], asr.at[p, c // step], partner)

    def send_amplitudes(p, lo=0, hi=None, both=False, wide=1):
        w, first, rows, n, step = pieces[p]
        size = wide * (G // n)
        span = pl.ds(first, rows)

        @pl.loop(lo // wide, (n if hi is None else hi) // wide)
        def _(c):
            part = pl.ds(c * size, size)
            lhs = cv[part, span].reshape(size * rows, M)
            if both:
                block = jnp.dot(lhs, th[w], preferred_element_type=F32).astype(BF16)
                asend[w, part, span] = block[:, R:].reshape(size, rows, R)
            else:
                block = jnp.dot(lhs, th[w, :, OTHER], preferred_element_type=F32).astype(BF16)
                asend[w, part, span] = block.reshape(size, rows, R)
            for k in range(wide):
                a_copy(p, c * wide + k).start()
            if both:
                adiag[w, part, span] = block[:, :R].reshape(size, rows, R)

        if lo == 0:
            drains.append(a_copy(p, 0, n).wait_send)

    GD = 2 * GC

    def diagonal(w, first, rows):
        size = min(G, GD * R // rows)
        span = pl.ds(first, rows)

        @pl.loop(0, G // size)
        def _(c):
            part = pl.ds(c * size, size)
            block = jnp.dot(cv[part, span].reshape(size * rows, M), th[w, :, OWN], preferred_element_type=F32)
            adiag[w, part, span] = block.astype(BF16).reshape(size, rows, R)

    def accumulate(stream, first, rows, block, part, size):
        lhs = jnp.concatenate([block[g] for g in range(size)], axis=1)
        for n in range(4):
            cols = pl.ds(n * Q, Q)
            acc[stream, pl.ds(first, rows), cols] += jnp.dot(
                lhs, cv[part, :, cols].reshape(size * R, Q), preferred_element_type=F32
            )

    def own_gradient(w):
        @pl.loop(0, G // GD)
        def _(c):
            part = pl.ds(c * GD, GD)
            accumulate(w, 0, R, adiag[w, part], part, GD)

    def swapped_gradient(p, lo=0, hi=None):
        w, first, rows, n, step = pieces[p]
        size = step * (G // n)

        @pl.loop(lo, n // step if hi is None else hi)
        def _(c):
            a_copy(p, c * step, step).wait_recv()
            part = pl.ds(c * size, size)
            accumulate(W + w, first, rows, arecv[w, part, pl.ds(first, rows)], part, size)

    class Scatter:
        def __init__(self, e):
            self.e = e
            self.stream, self.first, self.rows, self.direct = parts[e]
            self.span = pl.ds(self.first, self.rows)

        def own(self, d):
            return acc[self.stream, self.span, pl.ds(pl.multiple_of(d * Q, Q), Q)]

        def link(self, src, dst, k, to):
            return remote(src, dst, gss.at[self.e], gsr.at[self.e, k], on(to))

        def straight(self, k, to, slot=None):
            return self.link(gs.at[self.stream, k, self.span], gr.at[self.stream, k if slot is None else slot, self.span], 0, to)

        def to_near(self, k):
            return self.link(gs.at[self.stream, 1 + k, self.span], gf.at[self.stream, k, self.span], 1 + k, near)

        def across(self, k, to):
            return self.link(gc.at[self.stream, k, self.span], gr.at[self.stream, 1, self.span], 0, to)

        def arrived(self, count):
            return self.link(gs.at[self.stream, pl.ds(0, count), self.span], gr.at[self.stream, pl.ds(0, count), self.span], 0, mate)

        def to_owner(self, d):
            at = (self.stream, d, self.span)
            return remote(gs.at[at], gr.at[self.stream, z, self.span], gss.at[self.e], gsr.at[self.e, 0], {**partner, **on(d)})

        def to_owners(self):
            at = (self.stream, pl.ds(0, 4), self.span)
            return remote(gs.at[at], gr.at[at], gss.at[self.e], gsr.at[self.e, 0], partner)

        def start(self):
            if self.direct == 2:
                for d in range(4):
                    gs[self.stream, d, self.span] = self.own(d).astype(BF16)
                for k in (end, far, near, edge):
                    self.to_owner(k).start()
                drains.append(self.to_owners().wait_send)
                return
            if self.direct:
                for k, d in ((2, 3 - z), (1, 3 - mate), (0, mate)):
                    gs[self.stream, k, self.span] = self.own(d).astype(BF16)
                    self.straight(k, d).start()
            else:

                @pl.when(outer)
                def _():
                    for k, d in enumerate((far, end)):
                        gs[self.stream, 1 + k, self.span] = self.own(d).astype(BF16)
                        self.to_near(k).start()

                gs[self.stream, 0, self.span] = self.own(mate).astype(BF16)
                self.straight(0, mate).start()
            drains.append(self.arrived(3).wait_send)

        def relay(self):
            @pl.when(inner)
            def _():
                for k, d in enumerate((far, end)):
                    self.to_near(k).wait_recv()
                    gc[self.stream, k, self.span] = (self.own(d) + gf[self.stream, k, self.span].astype(F32)).astype(BF16)
                    self.across(k, d).start()

        def total(self):
            count = 3 if self.direct else 2
            self.arrived(count).wait_recv()
            total = self.own(z)
            for k in range(count):
                total += gr[self.stream, k, self.span].astype(F32)
            return total

    def x_copy(w, rows=None):
        if rows is None:
            rows = pl.ds(0, sum(size for stream, _, size, mode in parts if stream == W + w and mode < 2))
        return remote(xs.at[w, rows], xr.at[w, rows], xss.at[w], xsr.at[w], partner)

    def finish(e):
        stream, first, rows, _ = parts[e]
        total = scatters[e].total()
        if stream < W:
            gown[stream] = total
        else:
            w, span = stream - W, pl.ds(first, rows)
            xs[w, span] = total.astype(BF16)
            x_copy(w, span).start()
            if first == 0:
                drains.append(x_copy(w).wait_send)

    def settle(count=None):
        count = len(drains) if count is None else count
        for drain in drains[:count]:
            drain()
        del drains[:count]

    def store(w):
        x_copy(w).wait_recv()
        for e, (stream, first, rows, mode) in enumerate(parts):
            if stream == W + w:
                span = pl.ds(first, rows)
                if mode == 2:
                    scatters[e].to_owners().wait_recv()
                    for d in range(4):
                        gown[w, span] += gr[stream, d, span].astype(F32)
                else:
                    gown[w, span] += xr[w, span].astype(F32)
        out[w] = -gown[w].T

    scatters = [Scatter(e) for e in range(len(parts))]
    D0, D1, F0, G0, Fa, Fb, Fc = range(7)

    send_amplitudes(0, 0, 4, wide=2)
    for q in direct:
        own0.relay(q)
    crossed(1, Q).wait_recv()
    par1.start()
    own1.start()
    send_amplitudes(0, 4, 8, wide=2)
    for q in direct:
        own0.wait(q)
    send_amplitudes(1, both=True, wide=2)
    par1.relay()
    diagonal(0, 0, R // 2)
    own1.relay()
    own_gradient(0)
    scatters[D0].start()
    swapped_gradient(0)
    scatters[F0].start()
    par1.wait()
    own1.wait()
    send_amplitudes(2, both=True, wide=2)
    scatters[D0].relay()
    send_amplitudes(3, both=True, wide=2)
    send_amplitudes(4, both=True, wide=2)
    scatters[F0].relay()
    own_gradient(1)
    scatters[D1].start()
    swapped_gradient(1)
    scatters[G0].start()
    old = len(drains)
    finish(D0)
    swapped_gradient(2, 0, 2)
    scatters[D1].relay()
    swapped_gradient(2, 2, 4)
    scatters[Fa].start()
    swapped_gradient(3, 0, 2)
    scatters[G0].relay()
    swapped_gradient(3, 2, 4)
    scatters[Fb].start()
    swapped_gradient(4, 0, 2)
    scatters[Fa].relay()
    swapped_gradient(4, 2, 4)
    scatters[Fc].start()
    settle(old)
    finish(F0)
    finish(G0)
    finish(D1)
    finish(Fa)
    finish(Fb)
    finish(Fc)
    store(0)
    store(1)
    settle()


def fused(chol_half, theta):
    G, R, M = chol_half.shape
    W, Q, _ = theta.shape
    CH = 8
    NQ, NB = 4, 2
    H = R // 4
    modes = (0, 0, 0, 1, 1)
    pieces = ((0, 0, 2 * H, CH, 2), (0, 2 * H, 2 * H, CH, 2), (1, 0, 2 * H, 4, 1), (1, 2 * H, H, 4, 1), (1, 3 * H, H, 4, 1))
    parts = ((0, 0, R, 0), (1, 0, R, 0)) + tuple(
        (W + w, first, rows, mode) for (w, first, rows, _, _), mode in zip(pieces, modes)
    )
    dims = (G, R, M, W, Q, CH, NQ, NB, pieces, parts)
    E, PC = len(parts), len(pieces)
    dma = pltpu.SemaphoreType.DMA
    return pl.pallas_call(
        functools.partial(kernel, dims),
        out_shape=jax.ShapeDtypeStruct((W, Q, R), F32),
        in_specs=[pl.BlockSpec(memory_space=pl.ANY)] * 2,
        out_specs=pl.BlockSpec(memory_space=pltpu.VMEM),
        scratch_shapes=[
            pltpu.VMEM((G, R, M), BF16),
            pltpu.VMEM((W, M, 2 * R), BF16),
            pltpu.VMEM((W, G, R, R), BF16),
            pltpu.VMEM((W, G, R, R), BF16),
            pltpu.VMEM((W, G, R, R), BF16),
            pltpu.VMEM((2 * W, R, M), F32),
            pltpu.VMEM((2 * W, 4, R, Q), BF16),
            pltpu.VMEM((2 * W, 2, R, Q), BF16),
            pltpu.VMEM((2 * W, 2, R, Q), BF16),
            pltpu.VMEM((2 * W, 4, R, Q), BF16),
            pltpu.VMEM((W, R, Q), F32),
            pltpu.VMEM((W, R, Q), BF16),
            pltpu.VMEM((W, R, Q), BF16),
            dma,
            dma((W,)),
            dma((W,)),
            dma((W,)),
            dma((NQ,)),
            dma((4,)),
            dma((2, NQ, 3)),
            dma((2, 2)),
            dma((PC,)),
            dma((PC, 4)),
            dma((E,)),
            dma((E, 3)),
            dma((W,)),
            dma((W,)),
        ],
        compiler_params=pltpu.CompilerParams(collective_id=0, has_side_effects=True, vmem_limit_bytes=50000 << 10),
    )(chol_half, theta)


def on_device(mesh, chol_half, theta):
    G, R, M = chol_half.shape
    nz = mesh.shape["vec"]
    fits = theta.shape[0] == 2 and G % 16 == 0 and R == 128 and theta.shape[1] % 512 == 0 and G * R * M <= 8 << 20
    if mesh.shape["occ"] == 2 and nz == 4 and fits:
        return fused(chol_half, theta)
    widened = lax.all_gather(theta, "occ", axis=2, tiled=True)
    amplitude_sums = jnp.einsum(
        "gip,wpj->wgij", chol_half, lax.all_gather(widened, "vec", axis=1, tiled=True), preferred_element_type=F32
    )
    amplitudes = amplitude_sums.astype(BF16)
    swapped = lax.all_to_all(amplitudes, "occ", split_axis=3, concat_axis=2, tiled=True)
    summed_rows = lax.psum_scatter(
        jnp.einsum("gap,wgba->pwb", chol_half, swapped, preferred_element_type=F32),
        "vec",
        scatter_dimension=0,
        tiled=True,
    )
    owned = lax.psum_scatter(summed_rows, "occ", scatter_dimension=2, tiled=True)
    return -jnp.transpose(owned, (1, 0, 2))


def solution(mesh):
    return jax.shard_map(
        functools.partial(on_device, mesh),
        mesh=mesh,
        in_specs=(P(("grp", "vec"), "occ", None), P(("grp", "wlk"), "vec", "occ")),
        out_specs=P(("grp", "wlk"), "vec", "occ"),
        check_vma=False,
    )
```

```python
import functools

import jax
import jax.numpy as jnp
from jax import lax
from jax.experimental import pallas as pl
from jax.experimental.pallas import tpu as pltpu
from jax.sharding import PartitionSpec as P

MESH = pl.DeviceIdType.MESH
F32 = jnp.float32
BF16 = jnp.bfloat16


def kernel(dims, chol, theta, out, cv, th, asend, arecv, adiag, acc, gs, gf, gc, gr, gown, xs, xr,
           csem, tsem, txs, txr, txq, ags, agq, agr, ass, asr, gss, gsr, xss, xsr):
    G, R, M, W, Q, CH, NQ, NB, pieces, parts = dims
    z = lax.axis_index("vec")
    partner = {"occ": 1 - lax.axis_index("occ")}
    side = z // 2
    near, edge = 1 + side, 3 * side
    far, end = 3 - near, 3 - edge
    core = lax.axis_index("wlk")
    inner = z == near
    outer = z == edge
    mate = near + edge - z
    mine = pl.ds(pl.multiple_of(z * Q, Q), Q)
    GC = G // CH
    QC = Q // NQ

    drains = []

    def remote(src, dst, ss, rs, to):
        return pltpu.make_async_remote_copy(src_ref=src, dst_ref=dst, send_sem=ss, recv_sem=rs, device_id=to, device_id_type=MESH)

    def on(s):
        return {"vec": s}

    def c_copy(c):
        part = pl.ds(c * GC, GC)
        return pltpu.make_async_copy(chol.at[part], cv.at[part], csem)

    OWN, OTHER = pl.ds(0, R), pl.ds(R, R)

    def t_copy(w):
        return pltpu.make_async_copy(theta.at[w], th.at[w, mine, OWN], tsem.at[w])

    for w in range(W):
        t_copy(w).start()

    barrier = pltpu.get_barrier_semaphore()
    greeted = [partner]
    for k in range(1, 4):
        greeted.append(on(lax.rem(z + k, 4)))
    for device in greeted:
        pl.semaphore_signal(barrier, inc=1, device_id=device, device_id_type=MESH)
    pl.semaphore_wait(barrier, len(greeted))

    def rows_of(s, q, n):
        size = Q // n
        return pl.ds(pl.multiple_of(s * Q + q * size, size), size)

    def cross(w, rows):
        remote(th.at[w, rows, OWN], th.at[w, rows, OTHER], txs.at[w], txr.at[w], partner).start()

    def crossed(w, rows):
        rows = pl.ds(0, rows)
        return remote(th.at[w, rows, OWN], th.at[w, rows, OTHER], txs.at[w], txr.at[w], partner)

    def cross_first(q):
        rows = rows_of(z, q, NQ)
        return remote(th.at[0, rows, OWN], th.at[0, rows, OTHER], txs.at[0], txq.at[q], partner)

    class Gather:
        def __init__(self, s, columns, w, n):
            self.s, self.columns, self.w, self.n = s, columns, w, n

        def block(self, rows, recv, to):
            ref = th.at[self.w, rows, self.columns]
            return remote(ref, ref, ags.at[self.s], recv, on(to))

        def recv(self, q, kind):
            return agr.at[self.s, kind // 2] if self.n == 1 else agq.at[self.s - 2, q, kind]

        def copy(self, q, source, to, kind):
            return self.block(rows_of(source, q, self.n), self.recv(q, kind), to)

        def start(self, q=0):
            self.begin(q)
            drains.append(self.drain)

        def begin(self, q=0):
            own = functools.partial(self.copy, q, z)
            own(mate, 0).start()

            @pl.when(inner)
            def _():
                own(far, 1).start()
                own(end, 1).start()

            pl.when(outer)(lambda: own(far, 2).start())

        def arrive(self, q, source, kind):
            self.copy(q, source, mate, kind).wait_recv()

        def relay(self, q=0):
            @pl.when(inner)
            def _():
                self.arrive(q, end, 2)
                self.copy(q, end, edge, 2).start()

        def wait(self, q=0):
            if self.n == 1:
                self.block(pl.ds(0, 2 * Q), self.recv(0, 0), mate).wait_recv()
            else:
                self.arrive(q, mate, 0)
                self.arrive(q, far, 1)
            pl.when(outer)(lambda: self.arrive(q, end, 2))

        def drain(self):
            size = Q // self.n
            pl.when(inner)(lambda: self.block(pl.ds(0, 4 * size), self.recv(0, 0), mate).wait_send())
            pl.when(outer)(lambda: self.block(pl.ds(0, 2 * size), self.recv(0, 0), mate).wait_send())

    own0, par0, own1, par1 = Gather(2, OWN, 0, NQ), Gather(3, OTHER, 0, NQ), Gather(0, OWN, 1, 1), Gather(1, OTHER, 1, 1)
    direct, shared = range(NB, NQ), range(NB)

    t_copy(0).wait()
    for c in range(CH):
        c_copy(c).start()
    for q in direct:
        cross_first(q).start()
    for q in shared:
        own0.start(q)
        cross(0, rows_of(z, q, NQ))
    acc[...] = jnp.zeros_like(acc)
    t_copy(1).wait()
    cross(1, mine)
    drains.append(crossed(0, Q + 3 * NB * (Q // NQ)).wait_send)
    drains.append(crossed(1, Q).wait_send)
    for q in direct:
        cross_first(q).wait_recv()
        par0.start(q)
    for q in shared:
        for kind, source in enumerate((mate, far)):
            own0.arrive(q, source, kind)
            cross(0, rows_of(source, q, NQ))
        own0.relay(q)
        pl.when(inner)(lambda: cross(0, rows_of(end, q, NQ)))
    for q in direct:
        par0.relay(q)
    for q in shared:

        @pl.when(outer)
        def _():
            own0.arrive(q, end, 2)
            cross(0, rows_of(end, q, NQ))

    for q in direct:
        own0.start(q)
    for q in direct:
        par0.wait(q)
    pltpu.make_async_copy(chol, cv, csem).wait()
    crossed(0, 4 * NB * (Q // NQ)).wait_recv()

    def a_copy(p, c, count=1):
        w, first, rows, n, step = pieces[p]
        part = (w, pl.ds(c * (G // n), count * (G // n)), pl.ds(first, rows))
        return remote(asend.at[part], arecv.at[part], ass.at[p], asr.at[p, c // step], partner)

    def send_amplitudes(p, lo=0, hi=None, both=False, wide=1):
        w, first, rows, n, step = pieces[p]
        size = wide * (G // n)
        span = pl.ds(first, rows)

        @pl.loop(lo // wide, (n if hi is None else hi) // wide)
        def _(c):
            part = pl.ds(c * size, size)
            lhs = cv[part, span].reshape(size * rows, M)
            if both:
                block = jnp.dot(lhs, th[w], preferred_element_type=F32).astype(BF16)
                asend[w, part, span] = block[:, R:].reshape(size, rows, R)
            else:
                block = jnp.dot(lhs, th[w, :, OTHER], preferred_element_type=F32).astype(BF16)
                asend[w, part, span] = block.reshape(size, rows, R)
            for k in range(wide):
                a_copy(p, c * wide + k).start()
            if both:
                adiag[w, part, span] = block[:, :R].reshape(size, rows, R)

        if lo == 0:
            drains.append(a_copy(p, 0, n).wait_send)

    GD = 2 * GC

    def diagonal(w, first, rows):
        size = min(G, GD * R // rows)
        span = pl.ds(first, rows)

        @pl.loop(0, G // size)
        def _(c):
            part = pl.ds(c * size, size)
            block = jnp.dot(cv[part, span].reshape(size * rows, M), th[w, :, OWN], preferred_element_type=F32)
            adiag[w, part, span] = block.astype(BF16).reshape(size, rows, R)

    def accumulate(stream, first, rows, block, part, size):
        lhs = jnp.concatenate([block[g] for g in range(size)], axis=1)
        for n in range(4):
            cols = pl.ds(n * Q, Q)
            acc[stream, pl.ds(first, rows), cols] += jnp.dot(
                lhs, cv[part, :, cols].reshape(size * R, Q), preferred_element_type=F32
            )

    def own_gradient(w):
        @pl.loop(0, G // GD)
        def _(c):
            part = pl.ds(c * GD, GD)
            accumulate(w, 0, R, adiag[w, part], part, GD)

    def swapped_gradient(p, lo=0, hi=None):
        w, first, rows, n, step = pieces[p]
        size = step * (G // n)

        @pl.loop(lo, n // step if hi is None else hi)
        def _(c):
            a_copy(p, c * step, step).wait_recv()
            part = pl.ds(c * size, size)
            accumulate(W + w, first, rows, arecv[w, part, pl.ds(first, rows)], part, size)

    class Scatter:
        def __init__(self, e):
            self.e = e
            self.stream, self.first, self.rows, self.direct = parts[e]
            self.span = pl.ds(self.first, self.rows)

        def own(self, d):
            return acc[self.stream, self.span, pl.ds(pl.multiple_of(d * Q, Q), Q)]

        def link(self, src, dst, k, to):
            return remote(src, dst, gss.at[self.e], gsr.at[self.e, k], on(to))

        def straight(self, k, to, slot=None):
            return self.link(gs.at[self.stream, k, self.span], gr.at[self.stream, k if slot is None else slot, self.span], 0, to)

        def to_near(self, k):
            return self.link(gs.at[self.stream, 1 + k, self.span], gf.at[self.stream, k, self.span], 1 + k, near)

        def across(self, k, to):
            return self.link(gc.at[self.stream, k, self.span], gr.at[self.stream, 1, self.span], 0, to)

        def arrived(self, count):
            return self.link(gs.at[self.stream, pl.ds(0, count), self.span], gr.at[self.stream, pl.ds(0, count), self.span], 0, mate)

        def to_owner(self, d):
            at = (self.stream, d, self.span)
            return remote(gs.at[at], gr.at[self.stream, z, self.span], gss.at[self.e], gsr.at[self.e, 0], {**partner, **on(d)})

        def to_owners(self):
            at = (self.stream, pl.ds(0, 4), self.span)
            return remote(gs.at[at], gr.at[at], gss.at[self.e], gsr.at[self.e, 0], partner)

        def start(self):
            if self.direct == 2:
                for d in range(4):
                    gs[self.stream, d, self.span] = self.own(d).astype(BF16)
                for k in (end, far, near, edge):
                    self.to_owner(k).start()
                drains.append(self.to_owners().wait_send)
                return
            if self.direct:
                for k, d in ((2, 3 - z), (1, 3 - mate), (0, mate)):
                    gs[self.stream, k, self.span] = self.own(d).astype(BF16)
                    self.straight(k, d).start()
            else:

                @pl.when(outer)
                def _():
                    for k, d in enumerate((far, end)):
                        gs[self.stream, 1 + k, self.span] = self.own(d).astype(BF16)
                        self.to_near(k).start()

                gs[self.stream, 0, self.span] = self.own(mate).astype(BF16)
                self.straight(0, mate).start()
            drains.append(self.arrived(3).wait_send)

        def relay(self):
            @pl.when(inner)
            def _():
                for k, d in enumerate((far, end)):
                    self.to_near(k).wait_recv()
                    gc[self.stream, k, self.span] = (self.own(d) + gf[self.stream, k, self.span].astype(F32)).astype(BF16)
                    self.across(k, d).start()

        def total(self):
            count = 3 if self.direct else 2
            self.arrived(count).wait_recv()
            total = self.own(z)
            for k in range(count):
                total += gr[self.stream, k, self.span].astype(F32)
            return total

    def x_copy(w, rows=None):
        if rows is None:
            rows = pl.ds(0, sum(size for stream, _, size, mode in parts if stream == W + w and mode < 2))
        return remote(xs.at[w, rows], xr.at[w, rows], xss.at[w], xsr.at[w], partner)

    def finish(e):
        stream, first, rows, _ = parts[e]
        total = scatters[e].total()
        if stream < W:
            gown[stream] = total
        else:
            w, span = stream - W, pl.ds(first, rows)
            xs[w, span] = total.astype(BF16)
            x_copy(w, span).start()
            if first == 0:
                drains.append(x_copy(w).wait_send)

    def settle(count=None):
        count = len(drains) if count is None else count
        for drain in drains[:count]:
            drain()
        del drains[:count]

    def store(w):
        x_copy(w).wait_recv()
        for e, (stream, first, rows, mode) in enumerate(parts):
            if stream == W + w:
                span = pl.ds(first, rows)
                if mode == 2:
                    scatters[e].to_owners().wait_recv()
                    for d in range(4):
                        gown[w, span] += gr[stream, d, span].astype(F32)
                else:
                    gown[w, span] += xr[w, span].astype(F32)
        out[w] = -gown[w].T

    scatters = [Scatter(e) for e in range(len(parts))]
    D0, D1, F0, G0, Fa, Fb, Fc = range(7)

    send_amplitudes(0, 0, 4, wide=2)
    for q in direct:
        own0.relay(q)
    crossed(1, Q).wait_recv()
    par1.start()
    own1.start()
    send_amplitudes(0, 4, 8, wide=2)
    for q in direct:
        own0.wait(q)
    send_amplitudes(1, both=True, wide=2)
    par1.relay()
    diagonal(0, 0, R // 2)
    own1.relay()
    own_gradient(0)
    scatters[D0].start()
    swapped_gradient(0)
    scatters[F0].start()
    par1.wait()
    own1.wait()
    send_amplitudes(2, both=True, wide=2)
    scatters[D0].relay()
    send_amplitudes(3, both=True, wide=2)
    send_amplitudes(4, both=True, wide=2)
    scatters[F0].relay()
    own_gradient(1)
    scatters[D1].start()
    swapped_gradient(1)
    scatters[G0].start()
    old = len(drains)
    finish(D0)
    swapped_gradient(2, 0, 2)
    scatters[D1].relay()
    swapped_gradient(2, 2, 4)
    scatters[Fa].start()
    swapped_gradient(3, 0, 2)
    scatters[G0].relay()
    swapped_gradient(3, 2, 4)
    scatters[Fb].start()
    swapped_gradient(4, 0, 2)
    scatters[Fa].relay()
    swapped_gradient(4, 2, 4)
    scatters[Fc].start()
    settle(old)
    finish(F0)
    finish(G0)
    finish(D1)
    finish(Fa)
    finish(Fb)
    finish(Fc)
    store(0)
    store(1)
    settle()


def fused(chol_half, theta):
    G, R, M = chol_half.shape
    W, Q, _ = theta.shape
    CH = 8
    NQ, NB = 8, 4
    H = R // 4
    modes = (0, 0, 0, 1, 1)
    pieces = ((0, 0, 2 * H, CH, 2), (0, 2 * H, 2 * H, CH, 2), (1, 0, 2 * H, 4, 1), (1, 2 * H, H, 4, 1), (1, 3 * H, H, 4, 1))
    parts = ((0, 0, R, 0), (1, 0, R, 0)) + tuple(
        (W + w, first, rows, mode) for (w, first, rows, _, _), mode in zip(pieces, modes)
    )
    dims = (G, R, M, W, Q, CH, NQ, NB, pieces, parts)
    E, PC = len(parts), len(pieces)
    dma = pltpu.SemaphoreType.DMA
    return pl.pallas_call(
        functools.partial(kernel, dims),
        out_shape=jax.ShapeDtypeStruct((W, Q, R), F32),
        in_specs=[pl.BlockSpec(memory_space=pl.ANY)] * 2,
        out_specs=pl.BlockSpec(memory_space=pltpu.VMEM),
        scratch_shapes=[
            pltpu.VMEM((G, R, M), BF16),
            pltpu.VMEM((W, M, 2 * R), BF16),
            pltpu.VMEM((W, G, R, R), BF16),
            pltpu.VMEM((W, G, R, R), BF16),
            pltpu.VMEM((W, G, R, R), BF16),
            pltpu.VMEM((2 * W, R, M), F32),
            pltpu.VMEM((2 * W, 4, R, Q), BF16),
            pltpu.VMEM((2 * W, 2, R, Q), BF16),
            pltpu.VMEM((2 * W, 2, R, Q), BF16),
            pltpu.VMEM((2 * W, 4, R, Q), BF16),
            pltpu.VMEM((W, R, Q), F32),
            pltpu.VMEM((W, R, Q), BF16),
            pltpu.VMEM((W, R, Q), BF16),
            dma,
            dma((W,)),
            dma((W,)),
            dma((W,)),
            dma((NQ,)),
            dma((4,)),
            dma((2, NQ, 3)),
            dma((2, 2)),
            dma((PC,)),
            dma((PC, 4)),
            dma((E,)),
            dma((E, 3)),
            dma((W,)),
            dma((W,)),
        ],
        compiler_params=pltpu.CompilerParams(collective_id=0, has_side_effects=True, vmem_limit_bytes=50000 << 10),
    )(chol_half, theta)


def on_device(mesh, chol_half, theta):
    G, R, M = chol_half.shape
    nz = mesh.shape["vec"]
    fits = theta.shape[0] == 2 and G % 16 == 0 and R == 128 and theta.shape[1] % 512 == 0 and G * R * M <= 8 << 20
    if mesh.shape["occ"] == 2 and nz == 4 and fits:
        return fused(chol_half, theta)
    widened = lax.all_gather(theta, "occ", axis=2, tiled=True)
    amplitude_sums = jnp.einsum(
        "gip,wpj->wgij", chol_half, lax.all_gather(widened, "vec", axis=1, tiled=True), preferred_element_type=F32
    )
    amplitudes = amplitude_sums.astype(BF16)
    swapped = lax.all_to_all(amplitudes, "occ", split_axis=3, concat_axis=2, tiled=True)
    summed_rows = lax.psum_scatter(
        jnp.einsum("gap,wgba->pwb", chol_half, swapped, preferred_element_type=F32),
        "vec",
        scatter_dimension=0,
        tiled=True,
    )
    owned = lax.psum_scatter(summed_rows, "occ", scatter_dimension=2, tiled=True)
    return -jnp.transpose(owned, (1, 0, 2))


def solution(mesh):
    return jax.shard_map(
        functools.partial(on_device, mesh),
        mesh=mesh,
        in_specs=(P(("grp", "vec"), "occ", None), P(("grp", "wlk"), "vec", "occ")),
        out_specs=P(("grp", "wlk"), "vec", "occ"),
        check_vma=False,
    )
```
